16 devices in a mesh: dp: 2 (over y, z), tp: 8 (over x, core).
Axes of the slice: x: 4, y: 2, z: 1, core: 2. Of those that a mesh axis runs over, the one named last changes fastest.
The devices are a block of a 4x4x8 slice.
Arguments:
- x: bfloat16 [12, 2048, 3584], P('dp'), parts along dimension 0
- gamma: float32 [3584], replicated
- beta: float32 [3584], replicated
- wq: bfloat16 [3584, 4096], P(None, 'tp')
- wkv: bfloat16 [3584, 512], replicated
- wo: bfloat16 [4096, 3584], P('tp')
- w1: bfloat16 [3584, 14336], P(None, 'tp')
- w3: bfloat16 [3584, 14336], P(None, 'tp')
- w2: bfloat16 [14336, 3584], P('tp')
Outputs:
- output: bfloat16 [12, 2048, 3584], P('dp'), parts along dimension 0
There are 2 independent parts. The reference program is written for one: setup_inputs(seed, part) draws one part's arguments, and reference() takes and returns one part's arrays. A program takes and returns all parts, laid end to end along the dimension named above; an argument that names none is the same for every part.
All inputs are finite; a program needn't handle non-finite values.
Results may differ from the reference program's by a relative error of at most 0.0125647.
Values are sent between devices in bfloat16 or wider.
A program may use at most 768 MiB of HBM per device.

```python
import jax
import jax.numpy as jnp
from jax import lax
import math

D = 3584
HEADS = 16
HEAD = 256
FF = 14336
BATCH = 6
SEQ = 2048
EPS = 1e-5


def setup_inputs(seed: int = 0, part: int = 0) -> dict:
    key = jax.random.key(seed)
    ks = jax.random.split(key, 8)
    kx = jax.random.fold_in(jax.random.key(seed + 1), part)
    qscale = 0.85 * math.sqrt(max(1.0, math.log(SEQ / 32.0))) * D ** -0.5
    x = jax.random.normal(kx, (BATCH, SEQ, D), jnp.float32).astype(jnp.bfloat16)
    gamma = 1.0 + 0.3 * jax.random.normal(ks[0], (D,), jnp.float32)
    beta = 0.3 * jax.random.normal(ks[1], (D,), jnp.float32)
    wq = (qscale * jax.random.normal(ks[2], (D, HEADS * HEAD), jnp.float32)).astype(jnp.bfloat16)
    wkv = (D ** -0.5 * jax.random.normal(ks[3], (D, 2 * HEAD), jnp.float32)).astype(jnp.bfloat16)
    wo = (3.0 * (HEADS * HEAD) ** -0.5 * jax.random.normal(ks[4], (HEADS * HEAD, D), jnp.float32)).astype(jnp.bfloat16)
    w1 = (D ** -0.5 * jax.random.normal(ks[5], (D, FF), jnp.float32)).astype(jnp.bfloat16)
    w3 = (D ** -0.5 * jax.random.normal(ks[6], (D, FF), jnp.float32)).astype(jnp.bfloat16)
    w2 = (1.5 * FF ** -0.5 * jax.random.normal(ks[7], (FF, D), jnp.float32)).astype(jnp.bfloat16)
    return {'x': x, 'gamma': gamma, 'beta': beta, 'wq': wq, 'wkv': wkv, 'wo': wo, 'w1': w1, 'w3': w3, 'w2': w2}


def reference(x, gamma, beta, wq, wkv, wo, w1, w3, w2):
    qi = lax.broadcasted_iota(jnp.int32, (SEQ, SEQ), 0)
    ki = lax.broadcasted_iota(jnp.int32, (SEQ, SEQ), 1)
    causal = ki <= qi

    def one_seq(xs):
        xf = xs.astype(jnp.float32)
        mu = jnp.mean(xf, axis=-1, keepdims=True)
        var = jnp.mean(jnp.square(xf - mu), axis=-1, keepdims=True)
        ln = ((xf - mu) * lax.rsqrt(var + EPS) * gamma + beta).astype(jnp.bfloat16)
        q = jnp.dot(ln, wq, preferred_element_type=jnp.float32).astype(jnp.bfloat16)
        kv = jnp.dot(ln, wkv, preferred_element_type=jnp.float32).astype(jnp.bfloat16)
        k = kv[:, :HEAD]
        v = kv[:, HEAD:]

        def one_head(qh):
            s = jnp.dot(qh, k.T, preferred_element_type=jnp.float32) * HEAD ** -0.5
            s = jnp.where(causal, s, -1e30)
            p = jax.nn.softmax(s, axis=-1).astype(jnp.bfloat16)
            return jnp.dot(p, v, preferred_element_type=jnp.float32).astype(jnp.bfloat16)

        o = lax.map(one_head, q.reshape(SEQ, HEADS, HEAD).transpose(1, 0, 2))
        o = o.transpose(1, 0, 2).reshape(SEQ, HEADS * HEAD)
        a = jnp.dot(o, wo, preferred_element_type=jnp.float32)
        g = jnp.dot(ln, w1, preferred_element_type=jnp.float32)
        u = jnp.dot(ln, w3, preferred_element_type=jnp.float32)
        hm = (jax.nn.silu(g) * u).astype(jnp.bfloat16)
        m = jnp.dot(hm, w2, preferred_element_type=jnp.float32)
        return (xf + a + m).astype(jnp.bfloat16)

    return lax.map(one_seq, x)
```

```python
import functools

import jax
import jax.numpy as jnp
from jax import lax
from jax.experimental import pallas as pl
from jax.experimental.pallas import tpu as pltpu
from jax.sharding import PartitionSpec as P

EPS = 1e-5
F32, BF16 = jnp.float32, jnp.bfloat16
MESH = pl.DeviceIdType.MESH
LT = 128
CORES = 2


def layer_kernel(n_tok, seq, T, chips, x_hbm, g_ref, b_ref, wq_h, wkv_h, wo_h, w1_h, w3_h, w2_h, y_hbm, own_h, sib_h,
                 wqkv, w1, w3, w2o, lno, lns, kb, vb, qb, oh, pa_, pb_, q1, sb1, o2, s2, fo, fs, yb, r1, r2,
                 ss, ps, acc, ms, ls, al1,
                 wsem, xsem, o2sem, s2sem, fsem, osem, ds, dr, es, er, rs1_s, rs1_r, rs2_s, rs2_r,
                 ag1_s, ag1_r, ag2_s, ag2_r, lks, lkr, yw, ys, yr, credit, cr1, cr2):
    D = x_hbm.shape[1]
    dh = kb.shape[1]
    nh = wq_h.shape[1] // dh
    F = w1.shape[1]
    nb = seq // T
    n = n_tok // T
    H = T // CORES
    Q = H // chips
    C2 = 512 if D % 512 == 0 else 256
    nc2 = D // C2
    ns = max(nc2 * 2 // 7, 1)
    DA = ns * C2

    H2 = Q // 2
    tp = lax.axis_index('tp')
    core = lax.rem(tp, CORES)
    chip = lax.div(tp, CORES)
    nx = lax.rem(chip + 1, chips)
    pv_ = lax.rem(chip + chips - 1, chips)
    op = lax.rem(chip + 2, chips)
    nxt = {'tp': nx * CORES + core}
    prv = {'tp': pv_ * CORES + core}
    sib = {'tp': chip * CORES + (1 - core)}
    ways = ((nxt, nx, 0), (prv, pv_, 1))

    def prow(k):
        return pl.ds(pl.multiple_of(k * Q, Q), Q)

    def half_rows(b, c):
        return pl.ds(pl.multiple_of(b * T + c * H, H), H)

    def yrow(b, k, lo=0, nr=Q):
        return pl.ds(pl.multiple_of(b * T + core * H + k * Q + lo, H2), nr)

    def hrow(b, k):
        return pl.ds(pl.multiple_of(b * H + k * Q, Q), Q)

    def hblock(b):
        return pl.ds(pl.multiple_of(b * H, H), H)

    def valid(b):
        return (b >= 0) & (b < n)

    def remote(src, dst, ssem, rsem, dev):
        return pltpu.make_async_remote_copy(src_ref=src, dst_ref=dst, send_sem=ssem, recv_sem=rsem,
                                            device_id=dev, device_id_type=MESH)

    def local(src, dst, sem):
        return pltpu.make_async_copy(src, dst, sem)

    def signal(sem, dev):
        pl.semaphore_signal(sem, inc=1, device_id=dev, device_id_type=MESH)

    def two(b):
        return lax.rem(b + 8, 2)

    def three(b):
        return lax.rem(b + 9, 3)

    def four(b):
        return lax.rem(b + 8, 4)

    def eight(b):
        return lax.rem(b + 8, 8)

    def out_parts(ab):
        return ((pa_, 0, DA), (pb_, DA, D - DA))[ab]

    def out_own(b, ab):
        src, c0, cn = out_parts(ab)
        return local(src.at[pl.ds(0, H)], own_h.at[hblock(b), pl.ds(c0, cn)], osem.at[ab])

    def out_sib(b, ab):
        src, c0, cn = out_parts(ab)
        return remote(src.at[pl.ds(H, H)], sib_h.at[hblock(b), pl.ds(c0, cn)], ds.at[ab], dr.at[ab, four(b)], sib)

    def out_opp(b, ab):
        src, c0, cn = out_parts(ab)
        return remote(src.at[pl.ds(pl.multiple_of(H + op * Q, Q), Q)], sb1.at[two(b), :, pl.ds(c0, cn)],
                      es.at[ab], er.at[ab, four(b)], sib)

    def out_start(b, ab):
        @pl.when(valid(b))
        def _():
            out_opp(b, ab).start()
            out_own(b, ab).start()
            out_sib(b, ab).start()

    def out_wait(b):
        @pl.when(valid(b))
        def _():
            for ab in range(2):
                out_own(b, ab).wait()
                out_sib(b, ab).wait_send()
                out_opp(b, ab).wait_send()

    def pieces2(b, w):
        k = ways[w][1]
        return (local(own_h.at[hrow(b, k)], o2.at[w], o2sem.at[w]), local(sib_h.at[hrow(b, k)], s2.at[w], s2sem.at[w]))

    def pieces_f(b):
        return (local(own_h.at[hrow(b, chip)], fo, fsem.at[0]), local(sib_h.at[hrow(b, chip)], fs, fsem.at[1]),
                local(x_hbm.at[yrow(b, chip)], yb.at[two(b)], fsem.at[2]))

    def rs1_copy(b, w):
        dev, _, h = ways[w]
        return remote(q1.at[pl.ds(h * H2, H2)], r1.at[w], rs1_s.at[w], rs1_r.at[w], dev)

    def rs2_copy(b, w):
        return remote(o2.at[w], r2.at[two(b), w], rs2_s.at[w], rs2_r.at[w, two(b)], ways[w][0])

    def ag1_copy(b, w):
        return remote(yb.at[two(b)], y_hbm.at[yrow(b, chip)], ag1_s.at[w], ag1_r.at[w, eight(b)], ways[w][0])

    def ag2_copy(b, w):
        dev, _, h = ways[w]
        rows = yrow(b, ways[1 - w][1], h * H2, H2)
        return remote(y_hbm.at[rows], y_hbm.at[rows], ag2_s.at[w], ag2_r.at[w, eight(b)], dev)

    def yw_copy(b):
        return local(yb.at[two(b)], y_hbm.at[yrow(b, chip)], yw.at[0])

    def yd_copy(b):
        rows = half_rows(b, core)
        return remote(y_hbm.at[rows], y_hbm.at[rows], ys.at[0], yr.at[eight(b)], sib)

    def x_copy(b):
        return local(x_hbm.at[half_rows(b, core)], lno.at[three(b)], xsem.at[0])

    def own_kv(b):
        return pl.ds(pl.multiple_of(lax.rem(b, nb) * T, T), H)

    def sib_kv(b):
        return pl.ds(pl.multiple_of(lax.rem(b, nb) * T + H, H), H)

    def ln_copy(b):
        return remote(lno.at[three(b)], lns.at[two(b)], lks.at[0], lkr.at[two(b)], sib)

    def kv_copies(b):
        return (remote(kb.at[own_kv(b)], kb.at[sib_kv(b)], lks.at[1], lkr.at[2], sib),
                remote(vb.at[own_kv(b)], vb.at[sib_kv(b)], lks.at[2], lkr.at[3], sib))

    def w_copies(*which):
        srcs = [(wq_h, wqkv.at[:, pl.ds(0, nh * dh)]), (wkv_h, wqkv.at[:, pl.ds(nh * dh, 2 * dh)]), (w1_h, w1), (w3_h, w3),
                (wo_h, w2o.at[pl.ds(0, nh * dh)]), (w2_h, w2o.at[pl.ds(nh * dh, F)])]
        return [pltpu.make_async_copy(*srcs[i], wsem.at[i]) for i in which]

    def ln_rows(r0, b):
        sl = three(b)
        r = [pl.ds(pl.multiple_of(r0 + z, 16), 16) for z in (0, jnp.minimum(b, 0) * 16, jnp.minimum(b + 1, 0) * 16)]
        CW = 128
        cols = [pl.ds(c, CW) for c in range(0, D, CW)]
        tot = jnp.zeros((16, CW), F32)
        for c in cols:
            tot += lno[sl, r[0], c].astype(F32)
        mu = jnp.sum(tot, axis=1, keepdims=True) * (1.0 / D)
        sq = jnp.zeros((16, CW), F32)
        for c in cols:
            xc = lno[sl, r[1], c].astype(F32) - mu
            sq += xc * xc
        rstd = lax.rsqrt(jnp.sum(sq, axis=1, keepdims=True) * (1.0 / D) + EPS)
        for c in cols:
            lno[sl, r[2], c] = ((lno[sl, r[2], c].astype(F32) - mu) * rstd * g_ref[:, c] + b_ref[:, c]).astype(BF16)

    def kv_rows(b):
        kv = jnp.dot(lno[three(b)], wqkv[:, nh * dh:], preferred_element_type=F32)
        kb[own_kv(b), :] = kv[:, :dh].astype(BF16)
        vb[own_kv(b), :] = kv[:, dh:].astype(BF16)

    def lnv(b):
        return jnp.concatenate([lno[three(b)], lns[two(b)]], axis=0)

    def tick_a(t, main, last=False):
        if main:
            @pl.when(t >= 1)
            def _():
                signal(credit, sib)
            ln_copy(t).wait_send()

            @pl.when(t + 1 < n)
            def _():
                x_copy(t + 1).wait()
        if main or last:
            out_start(t - 1, 0)

        @pl.when(valid(t - 2))
        def _():
            for w in range(2):
                rs1_copy(t - 2, w).wait_recv()
                for c in pieces2(t - 2, w):
                    c.wait()

        @pl.when(valid(t - 3))
        def _():
            for w in range(2):
                rs2_copy(t - 3, w).wait_recv()
            for c in pieces_f(t - 3):
                c.wait()

    def tick_mid(t, main, last=False):
        if main or last:
            out_start(t - 1, 1)

        @pl.when(valid(t - 2))
        def _():
            for w in range(2):
                pl.semaphore_wait(cr2.at[w], 1)
                rs2_copy(t - 2, w).start()

        @pl.when(valid(t - 1))
        def _():
            for w in range(2):
                signal(cr1.at[w], ways[1 - w][0])
        if main:
            @pl.when(t >= 1)
            def _():
                pl.semaphore_wait(credit, 1)
                for c in kv_copies(t):
                    c.start()

            @pl.when(t + 1 < n)
            def _():
                ln_copy(t + 1).start()

            @pl.when(t + 2 < n)
            def _():
                x_copy(t + 2).start()
            ln_copy(t).wait_recv()

    SW = 256
    sum_cols = [pl.ds(c, SW) for c in range(0, D, SW)]

    def rs2_units(t):
        def unit(w, cs):
            def add():
                lo = ways[w][2] * H2
                for i in range(2):
                    rows = pl.ds(i * H2, H2)
                    if i * H2 == lo:
                        tot = o2[w, rows, cs].astype(F32) + s2[w, rows, cs].astype(F32) + r1[w, :, cs].astype(F32)
                        o2[w, rows, cs] = tot.astype(BF16)
                    else:
                        o2[w, rows, cs] = o2[w, rows, cs] + s2[w, rows, cs]
            return add
        return [unit(w, cs) for w in range(2) for cs in sum_cols]

    def final_units(t):
        s = two(t - 3)

        def unit(cs):
            def add():
                tot = r2[s, 0, :, cs].astype(F32) + r2[s, 1, :, cs].astype(F32)
                tot = tot + fo[:, cs].astype(F32) + fs[:, cs].astype(F32)
                yb[s, :, cs] = (yb[s, :, cs].astype(F32) + tot).astype(BF16)
            return add
        return [unit(cs) for cs in sum_cols]

    def run(units):
        for u in units:
            u()

    def tick_b(t, main):
        @pl.when(valid(t - 2))
        def _():
            for w in range(2):
                rs1_copy(t - 2, w).wait_send()

        @pl.when(valid(t - 1))
        def _():
            s = two(t - 1)
            for ab in range(2):
                out_opp(t - 1, ab).wait_recv()
                src, c0, cn = out_parts(ab)
                rows = prow(op)
                q1[:, pl.ds(c0, cn)] = src[rows, :] + sb1[s, :, pl.ds(c0, cn)]
            for w in range(2):
                pl.semaphore_wait(cr1.at[w], 1)
                rs1_copy(t - 1, w).start()
            for w in range(2):
                signal(cr2.at[w], ways[1 - w][0])

        @pl.when(valid(t - 5))
        def _():
            for w in range(2):
                ag2_copy(t - 5, w).wait_send()

        @pl.when(valid(t - 4))
        def _():
            for w in range(2):
                ag1_copy(t - 4, w).wait()
            yw_copy(t - 4).wait()
            for w in range(2):
                ag2_copy(t - 4, w).start()

        @pl.when(valid(t - 3))
        def _():
            for w in range(2):
                ag1_copy(t - 3, w).start()
            yw_copy(t - 3).start()

        @pl.when(valid(t - 6))
        def _():
            yd_copy(t - 6).wait()

        @pl.when(valid(t - 5))
        def _():
            for w in range(2):
                ag2_copy(t - 5, w).wait_recv()
            yd_copy(t - 5).start()

    def tick_c(t, main, last=False):
        if main or last:
            out_wait(t - 1)

        @pl.when(valid(t - 2))
        def _():
            for w in range(2):
                rs2_copy(t - 2, w).wait_send()

        @pl.when(valid(t - 1))
        def _():
            for ab in range(2):
                out_sib(t - 1, ab).wait_recv()
            for w in range(2):
                for c in pieces2(t - 1, w):
                    c.start()

        @pl.when(valid(t - 2))
        def _():
            for c in pieces_f(t - 2):
                c.start()
        if main:
            for c in kv_copies(t):
                c.wait_send()

    x_copy(0).start()
    for c in w_copies(*range(4)):
        c.start()
    vb[...] = jnp.zeros_like(vb)
    barrier = pltpu.get_barrier_semaphore()
    for dev in (nxt, prv, sib):
        pl.semaphore_signal(barrier, inc=1, device_id=dev, device_id_type=MESH)
    x_copy(0).wait()

    def ln_loop(i, _):
        ln_rows(pl.multiple_of(i * 16, 16), 0)
        return 0
    lax.fori_loop(0, H // 16, ln_loop, 0)
    x_copy(1).start()
    pl.semaphore_wait(barrier, 3)
    for c in w_copies(0, 1):
        c.wait()
    kv_rows(0)
    ln_copy(0).start()
    for c in kv_copies(0):
        c.start()

    NL = 2 * T // LT
    diff = lax.broadcasted_iota(jnp.int32, (T, LT), 1) - lax.rem(lax.broadcasted_iota(jnp.int32, (T, LT), 0) + core * H, T)

    def softmax(h, tiles):
        hs = pl.ds(h * T, T)
        mx = tiles[0]
        for a in tiles[1:]:
            mx = jnp.maximum(mx, a)
        m_old = ms[hs, :]
        m_new = jnp.maximum(m_old, jnp.max(mx, axis=1, keepdims=True))
        al = jnp.exp(m_old - m_new)
        ms[hs, :] = m_new
        ps_ = [jnp.exp(a - m_new) for a in tiles]
        tot = ps_[0]
        for a in ps_[1:]:
            tot = tot + a
        ls[hs, :] = ls[hs, :] * al + tot
        return jnp.concatenate(ps_, axis=1).astype(BF16), al

    def split(s):
        return [s[:, c * LT:(c + 1) * LT] for c in range(NL)]

    def pair(i):
        return pl.ds(pl.multiple_of(i * (2 * T), 2 * T), 2 * T)

    def qk(h, i):
        return lax.dot_general(qb[:, h * dh:(h + 1) * dh], kb[pair(i), :], (((1,), (1,)), ((), ())),
                               preferred_element_type=F32)

    def pv(h, p, al, i):
        hs = pl.ds(h * T, T)
        o = jnp.dot(p, vb[pair(i), :], preferred_element_type=F32)
        for c in range(dh // LT):
            cs = pl.ds(c * LT, LT)
            acc[hs, cs] = acc[hs, cs] * al + o[:, c * LT:(c + 1) * LT]

    C = 256
    nc = F // C

    def hidden(t, c):
        cs = pl.ds(c * C, C)
        g = jnp.dot(lnv(t), w1[:, cs], preferred_element_type=F32)
        u = jnp.dot(lnv(t), w3[:, cs], preferred_element_type=F32)
        oh[:, pl.ds(nh * dh + c * C, C)] = (g * (0.5 * jnp.tanh(0.5 * g) + 0.5) * u).astype(BF16)

    def out_chunk(c):
        a = jnp.dot(oh[...], w2o[:, pl.ds(c * C2, C2)], preferred_element_type=F32).astype(BF16)
        if c < ns:
            pa_[:, pl.ds(c * C2, C2)] = a
        else:
            pb_[:, pl.ds((c - ns) * C2, C2)] = a

    ne = min(4, nc - 1)

    def reset():
        acc[...] = jnp.zeros_like(acc)
        ls[...] = jnp.zeros_like(ls)
        ms[...] = jnp.full_like(ms, -1e30)
        al1[...] = jnp.ones_like(al1)
        ps[...] = jnp.zeros_like(ps)

    reset()

    def body(t, _):
        j = lax.rem(t, nb)
        npf = lax.div(j, 2)

        tick_a(t, True)

        us = rs2_units(t) + final_units(t)
        ng = H // 16
        for c in range(ns, nc2):
            out_chunk(c)
            for g in range((c - ns) * ng // (nc2 - ns), (c + 1 - ns) * ng // (nc2 - ns)):
                ln_rows(g * 16, t + 1)
            run(us[(c - ns) * len(us) // (nc2 - ns):(c + 1 - ns) * len(us) // (nc2 - ns)])

        tick_mid(t, True)

        @pl.when(t == 0)
        def _():
            for c in w_copies(2, 3):
                c.wait()

        q = jnp.dot(lnv(t), wqkv[:, 0:nh * dh], preferred_element_type=F32)
        qb[...] = (q.astype(BF16).astype(F32) * (dh ** -0.5)).astype(BF16)
        for c in range(ne):
            hidden(t, c)
            if c == ne - 3 or (ne < 3 and c == 0):
                for k in kv_copies(t):
                    k.wait_recv()
                ss[...] = qk(0, 0)

        tick_b(t, True)

        def attn(i, _):
            pv(1, ps[...], al1[...], jnp.maximum(i - 1, 0))
            s1 = qk(1, i)
            p0, al0 = softmax(0, split(ss))
            pv(0, p0, al0, i)
            ss[...] = qk(0, i + 1)
            p1, a1 = softmax(1, split(s1))
            ps[...] = p1
            al1[...] = a1
            return 0
        lax.fori_loop(0, npf, attn, 0)

        def masked(s):
            lim = lax.rem(j, 2) * T
            return [jnp.where(diff <= lim - ((c * LT) // T) * T - lax.rem((c * LT) % T + core * H, T), a, -1e30)
                    for c, a in enumerate(split(s))]

        def finish(h):
            hs = pl.ds(h * T, T)
            l = jnp.sum(ls[hs, :], axis=1, keepdims=True)
            oh[:, h * dh:(h + 1) * dh] = (acc[hs, :] / l).astype(BF16)

        tick_c(t, True)

        @pl.when(t == 0)
        def _():
            for c in w_copies(4, 5):
                c.start()

        pv(1, ps[...], al1[...], jnp.maximum(npf - 1, 0))
        hidden(t, ne)
        p0, al0 = softmax(0, masked(ss))
        pv(0, p0, al0, npf)
        ss[...] = qk(1, npf)
        for c in range(ne + 1, nc - 1):
            hidden(t, c)
        p1, a1 = softmax(1, masked(ss))
        pv(1, p1, a1, npf)
        for c in range(max(nc - 1, ne + 1), nc):
            hidden(t, c)
        kv_rows(t + 1)
        finish(0)
        finish(1)

        @pl.when(t == 0)
        def _():
            for c in w_copies(4, 5):
                c.wait()

        for c in range(ns):
            out_chunk(c)
            if c == 0:
                reset()
        return 0

    lax.fori_loop(0, n, body, 0)

    def rest(t, last):
        tick_a(t, False, last)
        if last:
            for c in range(ns, nc2):
                out_chunk(c)

        @pl.when(valid(t - 2))
        def _():
            run(rs2_units(t))

        @pl.when(valid(t - 3))
        def _():
            run(final_units(t))
        tick_mid(t, False, last)
        tick_b(t, False)
        tick_c(t, False, last)

    rest(n, True)

    def drain(t, _):
        rest(t, False)
        return 0
    lax.fori_loop(n + 1, n + 6, drain, 0)


def layer(mesh, x, gamma, beta, wq, wkv, wo, w1, w3, w2, T=256):
    b, s, d = x.shape
    dh = wkv.shape[1] // 2
    nh = wq.shape[1] // dh
    f = w1.shape[1]
    chips = mesh.shape['tp'] // CORES
    H = T // CORES
    Q = H // chips
    R = nh * T
    hbm = pl.BlockSpec(memory_space=pltpu.HBM)
    vm = pl.BlockSpec(memory_space=pltpu.VMEM)
    dma = pltpu.SemaphoreType.DMA
    reg = pltpu.SemaphoreType.REGULAR
    c2 = 512 if d % 512 == 0 else 256
    da = max(d // c2 * 2 // 7, 1) * c2
    assert chips == 4
    m = b * s
    flops = 2 * m * d * (wq.shape[1] + wkv.shape[1] + wo.shape[0] + 3 * f) + 2 * b * s * s * nh * dh
    res = pl.pallas_call(
        functools.partial(layer_kernel, m, s, T, chips),
        out_shape=[jax.ShapeDtypeStruct(o, BF16) for o in ((m, d), (m // CORES, d), (m // CORES, d))],
        in_specs=[hbm, vm, vm] + [hbm] * 6,
        out_specs=[hbm] * 3,
        scratch_shapes=[
            pltpu.VMEM((d, (nh + 2) * dh), BF16),
            pltpu.VMEM((d, f), BF16),
            pltpu.VMEM((d, f), BF16),
            pltpu.VMEM((nh * dh + f, d), BF16),
            pltpu.VMEM((3, H, d), BF16),
            pltpu.VMEM((2, H, d), BF16),
            pltpu.VMEM((s, dh), BF16),
            pltpu.VMEM((s, dh), BF16),
            pltpu.VMEM((T, nh * dh), BF16),
            pltpu.VMEM((T, nh * dh + f), BF16),
            pltpu.VMEM((T, da), BF16),
            pltpu.VMEM((T, d - da), BF16),
            pltpu.VMEM((Q, d), BF16),
            pltpu.VMEM((2, Q, d), BF16),
            pltpu.VMEM((2, Q, d), BF16),
            pltpu.VMEM((2, Q, d), BF16),
            pltpu.VMEM((Q, d), BF16),
            pltpu.VMEM((Q, d), BF16),
            pltpu.VMEM((2, Q, d), BF16),
            pltpu.VMEM((2, Q // 2, d), BF16),
            pltpu.VMEM((2, 2, Q, d), BF16),
            pltpu.VMEM((T, 2 * T), F32),
            pltpu.VMEM((T, 2 * T), BF16),
            pltpu.VMEM((R, dh), F32),
            pltpu.VMEM((R, LT), F32),
            pltpu.VMEM((R, LT), F32),
            pltpu.VMEM((T, LT), F32),
            dma((6,)), dma((1,)), dma((2,)), dma((2,)), dma((3,)), dma((2,)), dma((2,)), dma((2, 4)), dma((2,)), dma((2, 4)),
            dma((2,)), dma((2,)), dma((2,)), dma((2, 2)), dma((2,)), dma((2, 8)), dma((2,)), dma((2, 8)),
            dma((3,)), dma((4,)), dma((1,)), dma((1,)), dma((8,)),
            reg, reg((2,)), reg((2,)),
        ],
        compiler_params=pltpu.CompilerParams(vmem_limit_bytes=67043328, collective_id=0, has_side_effects=True),
        cost_estimate=pl.CostEstimate(flops=flops, bytes_accessed=6 * m * d, transcendentals=0),
        name='layer',
    )(x.reshape(m, d), gamma.reshape(1, d), beta.reshape(1, d), wq, wkv, wo, w1, w3, w2)
    return res[0].reshape(b, s, d)


def solution(mesh):
    return jax.shard_map(functools.partial(layer, mesh), mesh=mesh,
                         in_specs=(P('dp', None, None), P(), P(), P(None, 'tp'), P(), P('tp', None),
                                   P(None, 'tp'), P(None, 'tp'), P('tp', None)),
                         out_specs=P('dp', None, None), check_vma=False)
```

```python
import functools

import jax
import jax.numpy as jnp
from jax import lax
from jax.experimental import pallas as pl
from jax.experimental.pallas import tpu as pltpu
from jax.sharding import PartitionSpec as P

EPS = 1e-5
F32, BF16 = jnp.float32, jnp.bfloat16
MESH = pl.DeviceIdType.MESH
LT = 128
CORES = 2


def layer_kernel(n_tok, seq, T, chips, K, x_hbm, g_ref, b_ref, wq_h, wkv_h, wo_h, w1_h, w3_h, w2_h, y_hbm, own_h, sib_h, yp_h,
                 wqkv, w1, w3, w2o, lno, lns, kb, vb, qb, oh, pa_, pb_, q1, sb1, o2, s2, fo, fs, yb, r1, r2,
                 ss, ps, acc, ms, ls, al1,
                 wsem, xsem, o2sem, s2sem, fsem, osem, ds, dr, es, er, rs1_s, rs1_r, rs2_s, rs2_r,
                 ag1_s, ag1_r, ag2_s, ag2_r, lks, lkr, yw, ys, yr, credit, cr1, cr2):
    D = x_hbm.shape[1]
    dh = kb.shape[1]
    nh = wq_h.shape[1] // dh
    F = w1.shape[1]
    nb = seq // T
    n = n_tok // T
    H = T // CORES
    Q = H // chips
    C2 = 512 if D % 512 == 0 else 256
    nc2 = D // C2
    ns = max(nc2 * 2 // 7, 1)
    DA = ns * C2

    H2 = Q // 2
    tp = lax.axis_index('tp')
    core = lax.rem(tp, CORES)
    chip = lax.div(tp, CORES)
    nx = lax.rem(chip + 1, chips)
    pv_ = lax.rem(chip + chips - 1, chips)
    op = lax.rem(chip + 2, chips)
    nxt = {'tp': nx * CORES + core}
    prv = {'tp': pv_ * CORES + core}
    sib = {'tp': chip * CORES + (1 - core)}
    ways = ((nxt, nx, 0), (prv, pv_, 1))

    def prow(k):
        return pl.ds(pl.multiple_of(k * Q, Q), Q)

    def half_rows(b, c):
        return pl.ds(pl.multiple_of(b * T + c * H, H), H)

    def yrow(b, k, lo=0, nr=Q):
        return pl.ds(pl.multiple_of(b * T + core * H + k * Q + lo, H2), nr)

    def hrow(b, k):
        return pl.ds(pl.multiple_of(b * H + k * Q, Q), Q)

    def hblock(b):
        return pl.ds(pl.multiple_of(b * H, H), H)

    nk = n - K

    def valid(b):
        return (b >= 0) & (b < n)

    def spread(b):
        return (b >= 0) & (b < nk)

    def remote(src, dst, ssem, rsem, dev):
        return pltpu.make_async_remote_copy(src_ref=src, dst_ref=dst, send_sem=ssem, recv_sem=rsem,
                                            device_id=dev, device_id_type=MESH)

    def local(src, dst, sem):
        return pltpu.make_async_copy(src, dst, sem)

    def signal(sem, dev):
        pl.semaphore_signal(sem, inc=1, device_id=dev, device_id_type=MESH)

    def two(b):
        return lax.rem(b + 8, 2)

    def three(b):
        return lax.rem(b + 9, 3)

    def four(b):
        return lax.rem(b + 8, 4)

    def eight(b):
        return lax.rem(b + 8, 8)

    def out_parts(ab):
        return ((pa_, 0, DA), (pb_, DA, D - DA))[ab]

    def out_own(b, ab):
        src, c0, cn = out_parts(ab)
        return local(src.at[pl.ds(0, H)], own_h.at[hblock(b), pl.ds(c0, cn)], osem.at[ab])

    def out_sib(b, ab):
        src, c0, cn = out_parts(ab)
        return remote(src.at[pl.ds(H, H)], sib_h.at[hblock(b), pl.ds(c0, cn)], ds.at[ab], dr.at[ab, four(b)], sib)

    def out_opp(b, ab):
        src, c0, cn = out_parts(ab)
        return remote(src.at[pl.ds(pl.multiple_of(H + op * Q, Q), Q)], sb1.at[two(b), :, pl.ds(c0, cn)],
                      es.at[ab], er.at[ab, four(b)], sib)

    def out_start(b, ab):
        @pl.when(valid(b))
        def _():
            out_opp(b, ab).start()
            out_own(b, ab).start()
            out_sib(b, ab).start()

    def out_wait(b):
        @pl.when(valid(b))
        def _():
            for ab in range(2):
                out_own(b, ab).wait()
                out_sib(b, ab).wait_send()
                out_opp(b, ab).wait_send()

    def pieces2(b, w):
        k = ways[w][1]
        return (local(own_h.at[hrow(b, k)], o2.at[w], o2sem.at[w]), local(sib_h.at[hrow(b, k)], s2.at[w], s2sem.at[w]))

    def pieces_f(b):
        return (local(own_h.at[hrow(b, chip)], fo, fsem.at[0]), local(sib_h.at[hrow(b, chip)], fs, fsem.at[1]),
                local(x_hbm.at[yrow(b, chip)], yb.at[two(b)], fsem.at[2]))

    def rs1_copy(b, w):
        dev, _, h = ways[w]
        return remote(q1.at[pl.ds(h * H2, H2)], r1.at[w], rs1_s.at[w], rs1_r.at[w], dev)

    def rs2_copy(b, w):
        return remote(o2.at[w], r2.at[two(b), w], rs2_s.at[w], rs2_r.at[w, two(b)], ways[w][0])

    def ag1_copy(b, w):
        return remote(yb.at[two(b)], y_hbm.at[yrow(b, chip)], ag1_s.at[w], ag1_r.at[w, eight(b)], ways[w][0])

    def ag2_copy(b, w):
        dev, _, h = ways[w]
        rows = yrow(b, ways[1 - w][1], h * H2, H2)
        return remote(y_hbm.at[rows], y_hbm.at[rows], ag2_s.at[w], ag2_r.at[w, eight(b)], dev)

    def yw_copy(b):
        return local(yb.at[two(b)], y_hbm.at[yrow(b, chip)], yw.at[0])

    def yl_copy(b):
        return local(yb.at[two(b)], yp_h.at[pl.ds(pl.multiple_of((b - nk) * Q, Q), Q)], yw.at[0])

    def yd_copy(b):
        rows = half_rows(b, core)
        return remote(y_hbm.at[rows], y_hbm.at[rows], ys.at[0], yr.at[eight(b)], sib)

    def x_copy(b):
        return local(x_hbm.at[half_rows(b, core)], lno.at[three(b)], xsem.at[0])

    def own_kv(b):
        return pl.ds(pl.multiple_of(lax.rem(b, nb) * T, T), H)

    def sib_kv(b):
        return pl.ds(pl.multiple_of(lax.rem(b, nb) * T + H, H), H)

    def ln_copy(b):
        return remote(lno.at[three(b)], lns.at[two(b)], lks.at[0], lkr.at[two(b)], sib)

    def kv_copies(b):
        return (remote(kb.at[own_kv(b)], kb.at[sib_kv(b)], lks.at[1], lkr.at[2], sib),
                remote(vb.at[own_kv(b)], vb.at[sib_kv(b)], lks.at[2], lkr.at[3], sib))

    def w_copies(*which):
        srcs = [(wq_h, wqkv.at[:, pl.ds(0, nh * dh)]), (wkv_h, wqkv.at[:, pl.ds(nh * dh, 2 * dh)]), (w1_h, w1), (w3_h, w3),
                (wo_h, w2o.at[pl.ds(0, nh * dh)]), (w2_h, w2o.at[pl.ds(nh * dh, F)])]
        return [pltpu.make_async_copy(*srcs[i], wsem.at[i]) for i in which]

    def ln_rows(r0, b):
        sl = three(b)
        r = [pl.ds(pl.multiple_of(r0 + z, 16), 16) for z in (0, jnp.minimum(b, 0) * 16, jnp.minimum(b + 1, 0) * 16)]
        CW = 128
        cols = [pl.ds(c, CW) for c in range(0, D, CW)]
        tot = jnp.zeros((16, CW), F32)
        for c in cols:
            tot += lno[sl, r[0], c].astype(F32)
        mu = jnp.sum(tot, axis=1, keepdims=True) * (1.0 / D)
        sq = jnp.zeros((16, CW), F32)
        for c in cols:
            xc = lno[sl, r[1], c].astype(F32) - mu
            sq += xc * xc
        rstd = lax.rsqrt(jnp.sum(sq, axis=1, keepdims=True) * (1.0 / D) + EPS)
        for c in cols:
            lno[sl, r[2], c] = ((lno[sl, r[2], c].astype(F32) - mu) * rstd * g_ref[:, c] + b_ref[:, c]).astype(BF16)

    def kv_rows(b):
        kv = jnp.dot(lno[three(b)], wqkv[:, nh * dh:], preferred_element_type=F32)
        kb[own_kv(b), :] = kv[:, :dh].astype(BF16)
        vb[own_kv(b), :] = kv[:, dh:].astype(BF16)

    def lnv(b):
        return jnp.concatenate([lno[three(b)], lns[two(b)]], axis=0)

    def tick_a(t, main, last=False):
        if main:
            @pl.when(t >= 1)
            def _():
                signal(credit, sib)
            ln_copy(t).wait_send()

            @pl.when(t + 1 < n)
            def _():
                x_copy(t + 1).wait()
        if main or last:
            out_start(t - 1, 0)

        @pl.when(valid(t - 2))
        def _():
            for w in range(2):
                rs1_copy(t - 2, w).wait_recv()
                for c in pieces2(t - 2, w):
                    c.wait()

        @pl.when(valid(t - 3))
        def _():
            for w in range(2):
                rs2_copy(t - 3, w).wait_recv()
            for c in pieces_f(t - 3):
                c.wait()

    def tick_mid(t, main, last=False):
        if main or last:
            out_start(t - 1, 1)

        @pl.when(valid(t - 2))
        def _():
            for w in range(2):
                pl.semaphore_wait(cr2.at[w], 1)
                rs2_copy(t - 2, w).start()

        @pl.when(valid(t - 1))
        def _():
            for w in range(2):
                signal(cr1.at[w], ways[1 - w][0])
        if main:
            @pl.when(t >= 1)
            def _():
                pl.semaphore_wait(credit, 1)
                for c in kv_copies(t):
                    c.start()

            @pl.when(t + 1 < n)
            def _():
                ln_copy(t + 1).start()

            @pl.when(t + 2 < n)
            def _():
                x_copy(t + 2).start()
            ln_copy(t).wait_recv()

    SW = 256
    sum_cols = [pl.ds(c, SW) for c in range(0, D, SW)]

    def rs2_units(t):
        def unit(w, cs):
            def add():
                lo = ways[w][2] * H2
                for i in range(2):
                    rows = pl.ds(i * H2, H2)
                    if i * H2 == lo:
                        tot = o2[w, rows, cs].astype(F32) + s2[w, rows, cs].astype(F32) + r1[w, :, cs].astype(F32)
                        o2[w, rows, cs] = tot.astype(BF16)
                    else:
                        o2[w, rows, cs] = o2[w, rows, cs] + s2[w, rows, cs]
            return add
        return [unit(w, cs) for w in range(2) for cs in sum_cols]

    def final_units(t):
        s = two(t - 3)

        def unit(cs):
            def add():
                tot = r2[s, 0, :, cs].astype(F32) + r2[s, 1, :, cs].astype(F32)
                tot = tot + fo[:, cs].astype(F32) + fs[:, cs].astype(F32)
                yb[s, :, cs] = (yb[s, :, cs].astype(F32) + tot).astype(BF16)
            return add
        return [unit(cs) for cs in sum_cols]

    def run(units):
        for u in units:
            u()

    def tick_b(t, main):
        @pl.when(valid(t - 2))
        def _():
            for w in range(2):
                rs1_copy(t - 2, w).wait_send()

        @pl.when(valid(t - 1))
        def _():
            s = two(t - 1)
            for ab in range(2):
                out_opp(t - 1, ab).wait_recv()
                src, c0, cn = out_parts(ab)
                rows = prow(op)
                q1[:, pl.ds(c0, cn)] = src[rows, :] + sb1[s, :, pl.ds(c0, cn)]
            for w in range(2):
                pl.semaphore_wait(cr1.at[w], 1)
                rs1_copy(t - 1, w).start()
            for w in range(2):
                signal(cr2.at[w], ways[1 - w][0])

        @pl.when(spread(t - 5))
        def _():
            for w in range(2):
                ag2_copy(t - 5, w).wait_send()

        @pl.when(spread(t - 4))
        def _():
            for w in range(2):
                ag1_copy(t - 4, w).wait()
            yw_copy(t - 4).wait()
            for w in range(2):
                ag2_copy(t - 4, w).start()

        @pl.when((t - 4 >= nk) & (t - 4 < n))
        def _():
            yl_copy(t - 4).wait()

        @pl.when(spread(t - 3))
        def _():
            for w in range(2):
                ag1_copy(t - 3, w).start()
            yw_copy(t - 3).start()

        @pl.when((t - 3 >= nk) & (t - 3 < n))
        def _():
            yl_copy(t - 3).start()

        @pl.when(spread(t - 6))
        def _():
            yd_copy(t - 6).wait()

        @pl.when(spread(t - 5))
        def _():
            for w in range(2):
                ag2_copy(t - 5, w).wait_recv()
            yd_copy(t - 5).start()

    def tick_c(t, main, last=False):
        if main or last:
            out_wait(t - 1)

        @pl.when(valid(t - 2))
        def _():
            for w in range(2):
                rs2_copy(t - 2, w).wait_send()

        @pl.when(valid(t - 1))
        def _():
            for ab in range(2):
                out_sib(t - 1, ab).wait_recv()
            for w in range(2):
                for c in pieces2(t - 1, w):
                    c.start()

        @pl.when(valid(t - 2))
        def _():
            for c in pieces_f(t - 2):
                c.start()
        if main:
            for c in kv_copies(t):
                c.wait_send()

    x_copy(0).start()
    for c in w_copies(*range(4)):
        c.start()
    vb[...] = jnp.zeros_like(vb)
    barrier = pltpu.get_barrier_semaphore()
    for dev in (nxt, prv, sib):
        pl.semaphore_signal(barrier, inc=1, device_id=dev, device_id_type=MESH)
    x_copy(0).wait()

    def ln_loop(i, _):
        ln_rows(pl.multiple_of(i * 16, 16), 0)
        return 0
    lax.fori_loop(0, H // 16, ln_loop, 0)
    x_copy(1).start()
    pl.semaphore_wait(barrier, 3)
    for c in w_copies(0, 1):
        c.wait()
    kv_rows(0)
    ln_copy(0).start()
    for c in kv_copies(0):
        c.start()

    NL = 2 * T // LT
    diff = lax.broadcasted_iota(jnp.int32, (T, LT), 1) - lax.rem(lax.broadcasted_iota(jnp.int32, (T, LT), 0) + core * H, T)

    def softmax(h, tiles):
        hs = pl.ds(h * T, T)
        mx = tiles[0]
        for a in tiles[1:]:
            mx = jnp.maximum(mx, a)
        m_old = ms[hs, :]
        m_new = jnp.maximum(m_old, jnp.max(mx, axis=1, keepdims=True))
        al = jnp.exp(m_old - m_new)
        ms[hs, :] = m_new
        ps_ = [jnp.exp(a - m_new) for a in tiles]
        tot = ps_[0]
        for a in ps_[1:]:
            tot = tot + a
        ls[hs, :] = ls[hs, :] * al + tot
        return jnp.concatenate(ps_, axis=1).astype(BF16), al

    def split(s):
        return [s[:, c * LT:(c + 1) * LT] for c in range(NL)]

    def pair(i):
        return pl.ds(pl.multiple_of(i * (2 * T), 2 * T), 2 * T)

    def qk(h, i):
        return lax.dot_general(qb[:, h * dh:(h + 1) * dh], kb[pair(i), :], (((1,), (1,)), ((), ())),
                               preferred_element_type=F32)

    def pv(h, p, al, i):
        hs = pl.ds(h * T, T)
        o = jnp.dot(p, vb[pair(i), :], preferred_element_type=F32)
        for c in range(dh // LT):
            cs = pl.ds(c * LT, LT)
            acc[hs, cs] = acc[hs, cs] * al + o[:, c * LT:(c + 1) * LT]

    C = 256
    nc = F // C

    def hidden(t, c):
        cs = pl.ds(c * C, C)
        g = jnp.dot(lnv(t), w1[:, cs], preferred_element_type=F32)
        u = jnp.dot(lnv(t), w3[:, cs], preferred_element_type=F32)
        oh[:, pl.ds(nh * dh + c * C, C)] = (g * (0.5 * jnp.tanh(0.5 * g) + 0.5) * u).astype(BF16)

    def out_chunk(c):
        a = jnp.dot(oh[...], w2o[:, pl.ds(c * C2, C2)], preferred_element_type=F32).astype(BF16)
        if c < ns:
            pa_[:, pl.ds(c * C2, C2)] = a
        else:
            pb_[:, pl.ds((c - ns) * C2, C2)] = a

    ne = min(4, nc - 1)

    def reset():
        acc[...] = jnp.zeros_like(acc)
        ls[...] = jnp.zeros_like(ls)
        ms[...] = jnp.full_like(ms, -1e30)
        al1[...] = jnp.ones_like(al1)
        ps[...] = jnp.zeros_like(ps)

    reset()

    def body(t, _):
        j = lax.rem(t, nb)
        npf = lax.div(j, 2)

        tick_a(t, True)

        us = rs2_units(t) + final_units(t)
        ng = H // 16
        for c in range(ns, nc2):
            out_chunk(c)
            for g in range((c - ns) * ng // (nc2 - ns), (c + 1 - ns) * ng // (nc2 - ns)):
                ln_rows(g * 16, t + 1)
            run(us[(c - ns) * len(us) // (nc2 - ns):(c + 1 - ns) * len(us) // (nc2 - ns)])

        tick_mid(t, True)

        @pl.when(t == 0)
        def _():
            for c in w_copies(2, 3):
                c.wait()

        q = jnp.dot(lnv(t), wqkv[:, 0:nh * dh], preferred_element_type=F32)
        qb[...] = (q.astype(BF16).astype(F32) * (dh ** -0.5)).astype(BF16)
        for c in range(ne):
            hidden(t, c)
            if c == ne - 3 or (ne < 3 and c == 0):
                for k in kv_copies(t):
                    k.wait_recv()
                ss[...] = qk(0, 0)

        tick_b(t, True)

        def attn(i, _):
            pv(1, ps[...], al1[...], jnp.maximum(i - 1, 0))
            s1 = qk(1, i)
            p0, al0 = softmax(0, split(ss))
            pv(0, p0, al0, i)
            ss[...] = qk(0, i + 1)
            p1, a1 = softmax(1, split(s1))
            ps[...] = p1
            al1[...] = a1
            return 0
        lax.fori_loop(0, npf, attn, 0)

        def masked(s):
            lim = lax.rem(j, 2) * T
            return [jnp.where(diff <= lim - ((c * LT) // T) * T - lax.rem((c * LT) % T + core * H, T), a, -1e30)
                    for c, a in enumerate(split(s))]

        def finish(h):
            hs = pl.ds(h * T, T)
            l = jnp.sum(ls[hs, :], axis=1, keepdims=True)
            oh[:, h * dh:(h + 1) * dh] = (acc[hs, :] / l).astype(BF16)

        tick_c(t, True)

        @pl.when(t == 0)
        def _():
            for c in w_copies(4, 5):
                c.start()

        pv(1, ps[...], al1[...], jnp.maximum(npf - 1, 0))
        hidden(t, ne)
        p0, al0 = softmax(0, masked(ss))
        pv(0, p0, al0, npf)
        ss[...] = qk(1, npf)
        for c in range(ne + 1, nc - 1):
            hidden(t, c)
        p1, a1 = softmax(1, masked(ss))
        pv(1, p1, a1, npf)
        for c in range(max(nc - 1, ne + 1), nc):
            hidden(t, c)
        kv_rows(t + 1)
        finish(0)
        finish(1)

        @pl.when(t == 0)
        def _():
            for c in w_copies(4, 5):
                c.wait()

        for c in range(ns):
            out_chunk(c)
        ms[...] = jnp.full_like(ms, -1e30)
        return 0

    lax.fori_loop(0, n, body, 0)

    def rest(t, last):
        tick_a(t, False, last)
        if last:
            for c in range(ns, nc2):
                out_chunk(c)

        @pl.when(valid(t - 2))
        def _():
            run(rs2_units(t))

        @pl.when(valid(t - 3))
        def _():
            run(final_units(t))
        tick_mid(t, False, last)
        tick_b(t, False)
        tick_c(t, False, last)

    rest(n, True)

    def drain(t, _):
        rest(t, False)
        return 0
    lax.fori_loop(n + 1, max(nk + 6, n + 4), drain, 0)


def copy_kernel(R, NB, skip, src, dst, buf, isem, osem):
    n = (src.shape[0] - skip) // R
    ahead = NB // 2

    def rows(i):
        return pl.ds(pl.multiple_of(i * R, R), R)

    def get(i):
        return pltpu.make_async_copy(src.at[rows(i)], buf.at[lax.rem(i, NB)], isem.at[lax.rem(i, NB)])

    def put(i):
        return pltpu.make_async_copy(buf.at[lax.rem(i, NB)], dst.at[rows(i)], osem.at[lax.rem(i, NB)])

    for i in range(ahead):
        get(i).start()

    def step(i, _):
        get(i).wait()
        put(i).start()

        @pl.when(i + ahead < n)
        def _():
            @pl.when(i + ahead >= NB)
            def _():
                put(i + ahead - NB).wait()
            get(i + ahead).start()
        return 0
    lax.fori_loop(0, n, step, 0)

    def rest(i, _):
        put(i).wait()
        return 0
    lax.fori_loop(max(n - NB, 0), n, rest, 0)


def copy_rows(a, skip, R=256, NB=16):
    hbm = pl.BlockSpec(memory_space=pltpu.HBM)
    return pl.pallas_call(
        functools.partial(copy_kernel, R, NB, skip),
        out_shape=jax.ShapeDtypeStruct(a.shape, a.dtype),
        in_specs=[hbm],
        out_specs=hbm,
        scratch_shapes=[pltpu.VMEM((NB, R, a.shape[1]), a.dtype), pltpu.SemaphoreType.DMA((NB,)), pltpu.SemaphoreType.DMA((NB,))],
        compiler_params=pltpu.CompilerParams(vmem_limit_bytes=48 * 2 ** 20),
        cost_estimate=pl.CostEstimate(flops=10 ** 11, bytes_accessed=2 * a.size * 2, transcendentals=0),
        name='copy_rows',
    )(a)


def layer(mesh, x, gamma, beta, wq, wkv, wo, w1, w3, w2, T=256, K=3):
    b, s, d = x.shape
    dh = wkv.shape[1] // 2
    nh = wq.shape[1] // dh
    f = w1.shape[1]
    chips = mesh.shape['tp'] // CORES
    H = T // CORES
    Q = H // chips
    R = nh * T
    hbm = pl.BlockSpec(memory_space=pltpu.HBM)
    vm = pl.BlockSpec(memory_space=pltpu.VMEM)
    dma = pltpu.SemaphoreType.DMA
    reg = pltpu.SemaphoreType.REGULAR
    c2 = 512 if d % 512 == 0 else 256
    da = max(d // c2 * 2 // 7, 1) * c2
    assert chips == 4
    m = b * s
    flops = 2 * m * d * (wq.shape[1] + wkv.shape[1] + wo.shape[0] + 3 * f) + 2 * b * s * s * nh * dh
    res = pl.pallas_call(
        functools.partial(layer_kernel, m, s, T, chips, K),
        out_shape=[jax.ShapeDtypeStruct(o, BF16) for o in ((m, d), (m // CORES, d), (m // CORES, d), (K * Q, d))],
        in_specs=[hbm, vm, vm] + [hbm] * 6,
        out_specs=[hbm] * 4,
        scratch_shapes=[
            pltpu.VMEM((d, (nh + 2) * dh), BF16),
            pltpu.VMEM((d, f), BF16),
            pltpu.VMEM((d, f), BF16),
            pltpu.VMEM((nh * dh + f, d), BF16),
            pltpu.VMEM((3, H, d), BF16),
            pltpu.VMEM((2, H, d), BF16),
            pltpu.VMEM((s, dh), BF16),
            pltpu.VMEM((s, dh), BF16),
            pltpu.VMEM((T, nh * dh), BF16),
            pltpu.VMEM((T, nh * dh + f), BF16),
            pltpu.VMEM((T, da), BF16),
            pltpu.VMEM((T, d - da), BF16),
            pltpu.VMEM((Q, d), BF16),
            pltpu.VMEM((2, Q, d), BF16),
            pltpu.VMEM((2, Q, d), BF16),
            pltpu.VMEM((2, Q, d), BF16),
            pltpu.VMEM((Q, d), BF16),
            pltpu.VMEM((Q, d), BF16),
            pltpu.VMEM((2, Q, d), BF16),
            pltpu.VMEM((2, Q // 2, d), BF16),
            pltpu.VMEM((2, 2, Q, d), BF16),
            pltpu.VMEM((T, 2 * T), F32),
            pltpu.VMEM((T, 2 * T), BF16),
            pltpu.VMEM((R, dh), F32),
            pltpu.VMEM((R, LT), F32),
            pltpu.VMEM((R, LT), F32),
            pltpu.VMEM((T, LT), F32),
            dma((6,)), dma((1,)), dma((2,)), dma((2,)), dma((3,)), dma((2,)), dma((2,)), dma((2, 4)), dma((2,)), dma((2, 4)),
            dma((2,)), dma((2,)), dma((2,)), dma((2, 2)), dma((2,)), dma((2, 8)), dma((2,)), dma((2, 8)),
            dma((3,)), dma((4,)), dma((1,)), dma((1,)), dma((8,)),
            reg, reg((2,)), reg((2,)),
        ],
        compiler_params=pltpu.CompilerParams(vmem_limit_bytes=67043328, collective_id=0, has_side_effects=True),
        cost_estimate=pl.CostEstimate(flops=flops, bytes_accessed=6 * m * d, transcendentals=0),
        name='layer',
    )(x.reshape(m, d), gamma.reshape(1, d), beta.reshape(1, d), wq, wkv, wo, w1, w3, w2)
    last = lax.all_gather(res[3].reshape(K, Q, d), 'tp')
    y = copy_rows(res[0], K * T)
    last = last.reshape(chips, CORES, K, Q, d).transpose(2, 1, 0, 3, 4).reshape(K * T, d)
    return lax.dynamic_update_slice(y, last, (m - K * T, 0)).reshape(b, s, d)


def solution(mesh):
    return jax.shard_map(functools.partial(layer, mesh), mesh=mesh,
                         in_specs=(P('dp', None, None), P(), P(), P(None, 'tp'), P(), P('tp', None),
                                   P(None, 'tp'), P(None, 'tp'), P('tp', None)),
                         out_specs=P('dp', None, None), check_vma=False)
```
